32 devices in a mesh: col: 4 (over z), row: 8 (over y, x, core).
Axes of the slice: x: 2, y: 2, z: 4, core: 2. Of those that a mesh axis runs over, the one named last changes fastest.
Arguments:
- features: bfloat16 [65536, 384], P(('row', 'col'))
- w_hidden: bfloat16 [384, 512], replicated
- w_output: bfloat16 [512, 100], replicated
- adj_cols: int32 [32, 65536], P('col', 'row')
- adj_vals: bfloat16 [32, 65536], P('col', 'row')
- adj_mask: int32 [32, 65536], P('col', 'row')
- labels: int32 [65536], P(('row', 'col'))
- train_mask: int32 [65536], P(('row', 'col'))
Outputs:
- output 1: float32 [], replicated
- output 2: float32 [384, 512], replicated
- output 3: float32 [512, 100], replicated
All inputs are finite; a program needn't handle non-finite values.
Results may differ from the reference program's by a relative error of at most 0.00102.
Values are sent between devices in bfloat16 or wider.
A program may use at most 1 GiB of HBM per device.

```python
import jax
import jax.numpy as jnp
from jax import lax

NODES = 65536
FEAT = 384
HID = 512
CLS = 100
SLOTS = 32
COL_BLOCKS = 4
BLOCK_SLOTS = SLOTS // COL_BLOCKS
COL_NODES = NODES // COL_BLOCKS


def setup_inputs(seed: int = 0) -> dict:
    root_key = jax.random.key(seed)
    subkeys = jax.random.split(root_key, 8)
    adj_cols = jax.random.randint(subkeys[0], (SLOTS, NODES), 0, COL_NODES, dtype=jnp.int32)
    adj_mask = (jax.random.randint(subkeys[1], (SLOTS, NODES), 0, 4, dtype=jnp.int32) > 0).astype(jnp.int32)
    labels = jax.random.randint(subkeys[2], (NODES,), 0, CLS, dtype=jnp.int32)
    train_mask = jax.random.randint(subkeys[3], (NODES,), 0, 2, dtype=jnp.int32).at[0].set(1)
    degree = jnp.maximum(jnp.sum(adj_mask, axis=0), 1).astype(jnp.float32)
    spread = jax.random.uniform(subkeys[4], (SLOTS, NODES), jnp.float32, 0.5, 1.5)
    adj_vals = (spread * lax.rsqrt(degree)[None, :]).astype(jnp.bfloat16)
    features = jax.random.normal(subkeys[5], (NODES, FEAT), jnp.float32).astype(jnp.bfloat16)
    w_hidden = (jax.random.normal(subkeys[6], (FEAT, HID), jnp.float32) * FEAT ** -0.5).astype(jnp.bfloat16)
    w_output = (jax.random.normal(subkeys[7], (HID, CLS), jnp.float32) * HID ** -0.5).astype(jnp.bfloat16)
    return {"features": features, "w_hidden": w_hidden, "w_output": w_output, "adj_cols": adj_cols, "adj_vals": adj_vals, "adj_mask": adj_mask, "labels": labels, "train_mask": train_mask}


def gather_apply(global_cols, weights, dense):
    def slot_step(running, slot):
        col_ids, slot_w = slot
        return running + slot_w[:, None] * jnp.take(dense, col_ids, axis=0).astype(jnp.float32), None
    zero_acc = jnp.zeros((global_cols.shape[1], dense.shape[1]), jnp.float32)
    summed, _ = lax.scan(slot_step, zero_acc, (global_cols, weights))
    return summed


def scatter_apply(global_cols, weights, dense, num_out):
    dense_f = dense.astype(jnp.float32)
    def slot_step(running, slot):
        col_ids, slot_w = slot
        return running + jax.ops.segment_sum(slot_w[:, None] * dense_f, col_ids, num_segments=num_out), None
    zero_acc = jnp.zeros((num_out, dense.shape[1]), jnp.float32)
    summed, _ = lax.scan(slot_step, zero_acc, (global_cols, weights))
    return summed


def reference(features, w_hidden, w_output, adj_cols, adj_vals, adj_mask, labels, train_mask):
    offsets = (jnp.arange(SLOTS, dtype=jnp.int32) // BLOCK_SLOTS) * COL_NODES
    global_cols = adj_cols + offsets[:, None]
    weights = adj_vals.astype(jnp.float32) * adj_mask.astype(jnp.float32)
    proj_one = jnp.dot(features, w_hidden, preferred_element_type=jnp.float32).astype(jnp.bfloat16)
    z_one = gather_apply(global_cols, weights, proj_one).astype(jnp.bfloat16)
    h_one = jnp.maximum(z_one, 0)
    proj_two = jnp.dot(h_one, w_output, preferred_element_type=jnp.float32).astype(jnp.bfloat16)
    z_two = gather_apply(global_cols, weights, proj_two)
    mask_f = train_mask.astype(jnp.float32)
    train_count = jnp.maximum(jnp.sum(train_mask), 1).astype(jnp.float32)
    log_norm = jax.nn.logsumexp(z_two, axis=1)
    onehot = (labels[:, None] == jnp.arange(CLS, dtype=jnp.int32)[None, :]).astype(jnp.float32)
    picked = jnp.sum(z_two * onehot, axis=1)
    loss_mean = jnp.sum(mask_f * (log_norm - picked)) / train_count
    softmax_z = jnp.exp(z_two - log_norm[:, None])
    grad_two = ((mask_f / train_count)[:, None] * (softmax_z - onehot)).astype(jnp.bfloat16)
    back_two = scatter_apply(global_cols, weights, grad_two, NODES).astype(jnp.bfloat16)
    grad_w_output = jnp.dot(h_one.T, back_two, preferred_element_type=jnp.float32)
    dh_one = jnp.dot(back_two, w_output.T, preferred_element_type=jnp.float32)
    dz_one = jnp.where(z_one > 0, dh_one, 0.0).astype(jnp.bfloat16)
    back_one = scatter_apply(global_cols, weights, dz_one, NODES).astype(jnp.bfloat16)
    grad_w_hidden = jnp.dot(features.T, back_one, preferred_element_type=jnp.float32)
    return loss_mean, grad_w_hidden, grad_w_output
```

```python
import functools

import jax
import jax.numpy as jnp
from jax import lax
from jax.experimental import pallas as pl
from jax.experimental.pallas import tpu as pltpu
from jax.sharding import PartitionSpec as P

CONTRACT_ROWS = (((0,), (0,)), ((), ()))
CONTRACT_COLS = (((1,), (1,)), ((), ()))
LANES = 128
VMEM_LIMIT = 66 * 1000 * 1000
F32 = jnp.float32
BF16 = jnp.bfloat16


def gather_hidden_kernel(build_steps, tile, unroll, x_ref, w_ref, ids_ref, wts_ref, z_ref, table, total):
    phase, step = pl.program_id(0), pl.program_id(1)
    groups = w_ref.shape[1] // LANES
    in_rows = x_ref.shape[0]
    slots, rows = ids_ref.shape

    @pl.when(step < build_steps)
    def _():
        def build(t, carry):
            x = x_ref[pl.ds(pl.multiple_of(t * tile, tile), tile), :]
            base = (step * in_rows + t * tile) * groups
            y = jnp.dot(x, w_ref[...], preferred_element_type=F32).astype(BF16).astype(F32)
            for g in range(groups):
                table[pl.ds(base + g, tile, stride=groups), :] = y[:, g * LANES:(g + 1) * LANES]
            return carry
        lax.fori_loop(0, in_rows // tile, build, 0)

    @pl.when(step >= build_steps)
    def _():
        first = (step - build_steps) * rows

        def rows_of(t, carry):
            sums = []
            for u in range(unroll):
                r = t * unroll + u
                acc = None
                for s in range(slots):
                    row = table[pl.ds(pl.multiple_of(ids_ref[s, r], groups), groups), :]
                    term = wts_ref[s, r] * row
                    acc = term if acc is None else acc + term
                sums.append(acc)
            for u in range(unroll):
                at = pl.ds(pl.multiple_of((first + t * unroll + u) * groups, groups), groups)
                total[at, :] = jnp.where(phase > 0, total[at, :], 0.0) + sums[u]
            return carry
        lax.fori_loop(0, rows // unroll, rows_of, 0)

        @pl.when(phase == pl.num_programs(0) - 1)
        def _():
            def finish(t, carry):
                start = pl.multiple_of(first + t * tile, tile)
                for g in range(groups):
                    part = total[pl.ds(start * groups + g, tile, stride=groups), :]
                    z_ref[pl.ds(start, tile), g * LANES:(g + 1) * LANES] = part.astype(BF16)
                return carry
            lax.fori_loop(0, rows // tile, finish, 0)


def gather_hidden(x_all, w_hidden, ids, wts):
    phases, slots = 4, ids.shape[0] // 4
    nodes, feat = x_all.shape
    hid = w_hidden.shape[1]
    groups = hid // LANES
    rows = ids.shape[1]
    block_nodes = nodes // phases
    in_rows, row_block = 2048, 512
    build_steps, gather_steps = block_nodes // in_rows, rows // row_block
    edge_spec = pl.BlockSpec((slots, row_block), lambda p, s: (p, jnp.maximum(s - build_steps, 0)), memory_space=pltpu.SMEM)
    return pl.pallas_call(
        functools.partial(gather_hidden_kernel, build_steps, 256, 4),
        grid=(phases, build_steps + gather_steps),
        out_shape=jax.ShapeDtypeStruct((rows, hid), BF16),
        in_specs=[
            pl.BlockSpec((in_rows, feat), lambda p, s: (p * build_steps + jnp.minimum(s, build_steps - 1), 0)),
            pl.BlockSpec((feat, hid), lambda p, s: (0, 0)),
            edge_spec,
            edge_spec,
        ],
        out_specs=pl.BlockSpec((rows, hid), lambda p, s: (0, 0)),
        scratch_shapes=[pltpu.VMEM((block_nodes * groups, LANES), F32), pltpu.VMEM((rows * groups, LANES), F32)],
        compiler_params=pltpu.CompilerParams(vmem_limit_bytes=VMEM_LIMIT, dimension_semantics=("arbitrary", "arbitrary")),
        name="gather_hidden",
    )(x_all, w_hidden, ids, wts)


def gather_class_kernel(build_steps, tile, unroll, p_ref, ids_ref, wts_ref, z_ref, table):
    step = pl.program_id(0)
    in_rows = p_ref.shape[0]
    slots, rows = ids_ref.shape

    @pl.when(step < build_steps)
    def _():
        def build(t, carry):
            at = pl.multiple_of(t * tile, tile)
            table[pl.ds(pl.multiple_of(step * in_rows + at, tile), tile), :] = p_ref[pl.ds(at, tile), :].astype(F32)
            return carry
        lax.fori_loop(0, in_rows // tile, build, 0)

    @pl.when(step >= build_steps)
    def _():
        first = (step - build_steps) * rows

        def rows_of(t, carry):
            for u in range(unroll):
                r = t * unroll + u
                accs = [None, None]
                for s in range(slots):
                    term = wts_ref[s, r] * table[pl.ds(ids_ref[s, r], 1), :]
                    accs[s % 2] = term if accs[s % 2] is None else accs[s % 2] + term
                z_ref[pl.ds(first + r, 1), :] = accs[0] + accs[1]
            return carry
        lax.fori_loop(0, rows // unroll, rows_of, 0)


def gather_class(p_all, ids, wts):
    nodes, width = p_all.shape
    slots, rows = ids.shape
    in_rows, row_block = 8192, 256
    build_steps, gather_steps = nodes // in_rows, rows // row_block
    edge_spec = pl.BlockSpec((slots, row_block), lambda s: (0, jnp.maximum(s - build_steps, 0)), memory_space=pltpu.SMEM)
    return pl.pallas_call(
        functools.partial(gather_class_kernel, build_steps, 256, 2),
        grid=(build_steps + gather_steps,),
        out_shape=jax.ShapeDtypeStruct((rows, width), F32),
        in_specs=[pl.BlockSpec((in_rows, width), lambda s: (jnp.minimum(s, build_steps - 1), 0)), edge_spec, edge_spec],
        out_specs=pl.BlockSpec((rows, width), lambda s: (0, 0)),
        scratch_shapes=[pltpu.VMEM((nodes, width), F32)],
        compiler_params=pltpu.CompilerParams(vmem_limit_bytes=VMEM_LIMIT, dimension_semantics=("arbitrary",)),
        name="gather_class",
    )(p_all, ids, wts)


HALF = 128


def scatter_kernel(groups, pairs, same_ref, ids_ref, wts_ref, d_ref, out_ref, rows_f, acc, sem):
    step = pl.program_id(0)
    slots, rows = ids_ref.shape

    @pl.when(step == 0)
    def _():
        def clear(t, carry):
            acc[pl.ds(pl.multiple_of(t * 256, 256), 256), :] = jnp.zeros((256, LANES), F32)
            return carry
        lax.fori_loop(0, acc.shape[0] // 256, clear, 0)

    for g in range(groups):
        rows_f[pl.ds(g, rows, stride=groups), :] = d_ref[:, g * LANES:(g + 1) * LANES].astype(F32)

    def at_of(s, r):
        return pl.ds(pl.multiple_of(ids_ref[s, r], groups), groups)

    def source(r):
        return rows_f[pl.ds(pl.multiple_of(r * groups, groups), groups), :]

    for block in range(rows // (2 * HALF)):
        def batch(t, carry):
            same = same_ref[block, t * pairs]
            for k in range(1, pairs):
                same = same + same_ref[block, t * pairs + k]

            @pl.when(same == 0)
            def _():
                for k in range(pairs):
                    both = (block * 2 * HALF + t * pairs + k, block * 2 * HALF + HALF + t * pairs + k)
                    places, sums = [], []
                    for r in both:
                        d = source(r)
                        for s in range(slots):
                            at = at_of(s, r)
                            places.append(at)
                            sums.append(acc[at, :] + wts_ref[s, r] * d)
                    for at, value in zip(places, sums):
                        acc[at, :] = value

            @pl.when(same != 0)
            def _():
                for k in range(pairs):
                    for h in range(2):
                        r = block * 2 * HALF + h * HALF + t * pairs + k
                        d = source(r)

                        def one(s, c):
                            at = at_of(s, r)
                            acc[at, :] = acc[at, :] + wts_ref[s, r] * d
                            return c
                        lax.fori_loop(0, slots, one, 0)
            return carry
        lax.fori_loop(0, HALF // pairs, batch, 0)

    @pl.when(step == pl.num_programs(0) - 1)
    def _():
        copy = pltpu.make_async_copy(acc, out_ref, sem)
        copy.start()
        copy.wait()


def scatter_rows(same, ids, wts, dense, num_out):
    slots, rows = ids.shape
    groups = dense.shape[1] // LANES
    row_block = 1024
    blocks = row_block // (2 * HALF)
    edge_spec = pl.BlockSpec((slots, row_block), lambda s: (0, s), memory_space=pltpu.SMEM)
    return pl.pallas_call(
        functools.partial(scatter_kernel, groups, 2),
        grid=(rows // row_block,),
        out_shape=jax.ShapeDtypeStruct((num_out * groups, LANES), F32),
        in_specs=[
            pl.BlockSpec((None, blocks, HALF), lambda s: (s, 0, 0), memory_space=pltpu.SMEM),
            edge_spec,
            edge_spec,
            pl.BlockSpec((row_block, groups * LANES), lambda s: (s, 0)),
        ],
        out_specs=pl.BlockSpec(memory_space=pl.ANY),
        scratch_shapes=[
            pltpu.VMEM((row_block * groups, LANES), F32),
            pltpu.VMEM((num_out * groups, LANES), F32),
            pltpu.SemaphoreType.DMA,
        ],
        compiler_params=pltpu.CompilerParams(vmem_limit_bytes=VMEM_LIMIT, dimension_semantics=("arbitrary",)),
        name=f"scatter_rows_{groups}",
    )(same.reshape(rows // row_block, blocks, HALF), ids, wts, dense)


def shared_ids(ids):
    slots, rows = ids.shape
    blocks = ids.reshape(slots, rows // (2 * HALF), 2, HALF)
    each = [blocks[s, :, h] for s in range(slots) for h in range(2)]
    same = jnp.zeros(each[0].shape, jnp.bool_)
    for a in range(len(each)):
        for b in range(a):
            same = same | (each[a] == each[b])
    return same.astype(jnp.int32)


def solution(mesh):
    row_size = mesh.shape["row"]
    col_size = mesh.shape["col"]
    both_axes = ("col", "row")
    node_axes = ("row", "col")
    to_dest = [(flat_idx, (flat_idx % col_size) * row_size + flat_idx // col_size) for flat_idx in range(row_size * col_size)]

    def device_step(feat_blk, w_hidden, w_output, cols_blk, vals_blk, mask_blk, labels_blk, train_blk):
        blk_nodes = feat_blk.shape[0]
        col_nodes = blk_nodes * row_size
        slots = cols_blk.shape[0]
        hid, classes = w_output.shape
        groups = hid // LANES
        masked = jnp.where(mask_blk > 0, vals_blk, jnp.zeros_like(vals_blk))
        weights = masked.astype(F32)
        w_out = jnp.pad(w_output, ((0, 0), (0, LANES - classes)))
        lane = jnp.arange(LANES, dtype=jnp.int32)[None, :]

        x_all = lax.all_gather(feat_blk, node_axes, axis=0, tiled=True)
        own_ids = lax.all_to_all(cols_blk.reshape(slots, col_size, blk_nodes), "col", 1, 0).reshape(slots * col_size, blk_nodes)
        own_wts = lax.all_to_all(masked.reshape(slots, col_size, blk_nodes), "col", 1, 0).reshape(slots * col_size, blk_nodes).astype(F32)
        same = shared_ids(cols_blk)

        z_one = gather_hidden(x_all, w_hidden, own_ids * groups, own_wts)
        h_one = jnp.maximum(z_one, 0)
        proj_two = jnp.dot(h_one, w_out, preferred_element_type=F32).astype(BF16)
        count = jnp.sum(train_blk)
        extra = jnp.where(lane == classes, count // 64, jnp.where(lane == classes + 1, count % 64, 0)).astype(BF16)
        proj_two = jnp.where(lane < classes, proj_two, extra)
        p_all = lax.all_gather(proj_two, node_axes, axis=0, tiled=True)
        counts = p_all.reshape(row_size * col_size, blk_nodes, LANES)[:, 0, classes:classes + 2].astype(F32)
        train_count = jnp.maximum(jnp.sum(counts[:, 0] * 64.0 + counts[:, 1]), 1.0)

        starts = (jnp.arange(slots * col_size, dtype=jnp.int32) // slots) * col_nodes
        z_two = gather_class(p_all, own_ids + starts[:, None], own_wts)
        mask_f = train_blk.astype(F32)
        z_two = jnp.where(lane < classes, z_two, -jnp.inf)
        peak = jnp.max(z_two, axis=1, keepdims=True)
        exps = jnp.exp(z_two - peak)
        log_norm = jnp.log(jnp.sum(exps, axis=1, keepdims=True)) + peak
        onehot = labels_blk[:, None] == lane
        picked = jnp.sum(jnp.where(onehot, z_two, 0.0), axis=1)
        loss_part = jnp.sum(mask_f * (log_norm[:, 0] - picked)) / train_count
        softmax_z = jnp.exp(z_two - log_norm)
        grad_two = ((mask_f / train_count)[:, None] * (softmax_z - onehot.astype(F32))).astype(BF16)

        grad_rows = lax.all_gather(grad_two, "col", axis=0, tiled=True)
        part_back = scatter_rows(same, cols_blk, weights, grad_rows, col_nodes)
        back_src = lax.psum_scatter(part_back, "row", scatter_dimension=0, tiled=True).astype(BF16)
        back_two = lax.ppermute(back_src, both_axes, to_dest)
        grad_w_output = lax.dot_general(h_one, back_two, CONTRACT_ROWS, preferred_element_type=F32)
        dh_one = lax.dot_general(back_two, w_out, CONTRACT_COLS, preferred_element_type=F32)
        dz_one = jnp.where(z_one > 0, dh_one, 0.0).astype(BF16)
        dz_rows = lax.all_gather(dz_one, "col", axis=0, tiled=True)
        part_dz = scatter_rows(same, cols_blk * groups, weights, dz_rows, col_nodes)
        back_one = lax.psum_scatter(part_dz, "row", scatter_dimension=0, tiled=True).astype(BF16).reshape(blk_nodes, hid)
        src_blk = lax.axis_index("col") * row_size + lax.axis_index("row")
        feat_src = lax.dynamic_slice_in_dim(x_all, src_blk * blk_nodes, blk_nodes, axis=0)
        grad_w_hidden = lax.dot_general(feat_src, back_one, CONTRACT_ROWS, preferred_element_type=F32)
        tail = jnp.where((lane == classes) & (jnp.arange(hid)[:, None] == 0), loss_part, 0.0)
        grad_w_output = jnp.where(lane < classes, grad_w_output, tail)
        grad_w_hidden, grad_w_output = lax.psum((grad_w_hidden, grad_w_output), both_axes)
        return grad_w_output[0, classes], grad_w_hidden, grad_w_output[:, :classes]

    node_spec = P(("row", "col"), None)
    label_spec = P(("row", "col"))
    adj_spec = P("col", "row")
    return jax.shard_map(device_step, mesh=mesh, in_specs=(node_spec, P(), P(), adj_spec, adj_spec, adj_spec, label_spec, label_spec), out_specs=(P(), P(), P()), check_vma=False)
```
